32 devices in a mesh: slides: 2 (over x), rows: 8 (over z, y), cols: 2 (over core).
Axes of the slice: x: 2, y: 2, z: 4, core: 2. Of those that a mesh axis runs over, the one named last changes fastest.
Arguments:
- image: bfloat16 [512, 512, 128], P(('slides', 'rows'), 'cols'), parts along dimension 0, may hold values from -6 to 6
- tissue: int32 [16, 16], P(('slides', 'rows'), 'cols'), parts along dimension 0, may hold values 0 or 1
- first_kernel: bfloat16 [3, 3, 128, 128], replicated, may hold values from -0.1875 to 0.1875
- first_bias: float32 [128], replicated, may hold values from -3 to 3
- second_kernel: bfloat16 [3, 3, 128, 128], replicated, may hold values from -0.1875 to 0.1875
- second_bias: float32 [128], replicated, may hold values from -3 to 3
Outputs:
- features: bfloat16 [512, 512, 128], P(('slides', 'rows'), 'cols'), parts along dimension 0
The draws below stay inside these ranges and needn't reach their ends.
There are 2 independent parts, one for each index of `slides`. The reference program is written for one: setup_inputs(seed, part) draws one part's arguments, and reference() takes and returns one part's arrays. A program takes and returns all parts, laid end to end along the dimension named above; an argument that names none is the same for every part. Nothing has to cross between parts.
All inputs are finite; a program needn't handle non-finite values. No bound on the sum of `tissue` on one device may be relied on, other than what follows from the above.
Results may differ from the reference program's by a relative error of at most 0.0043.
Values may be sent and summed in bfloat16 or wider, within the bound.
A program may use at most 128 MiB of HBM per device.

```python
import jax
import jax.numpy as jnp

C = 128
MB = 32
H = 256
W = 512


def place_ends(array, own_key, least, high):
    longest = array.shape.index(max(array.shape))
    spots = []
    for shift in (0, 1):
        where = [jax.random.randint(jax.random.fold_in(own_key, axis), (), 0, length) for axis, length in enumerate(array.shape)]
        where[longest] = (where[longest] + shift) % array.shape[longest]
        spots.append(tuple(where))
    return array.at[spots[0]].set(least).at[spots[1]].set(high)


def block_scale(own_key, shape, shards, low, top_value):
    loudness, own = 1.0, jax.random.fold_in(own_key, 6)
    for position, parts in shards:
        steps = jnp.exp(jax.random.uniform(jax.random.fold_in(own, position), (parts,), jnp.float32, low / len(shards), top_value / len(shards)))
        loudness = loudness * jnp.repeat(steps, shape[position] // parts).reshape([-1 if axis == position else 1 for axis in range(len(shape))])
    return loudness


def normal_values(stream_key, dims, spread, bound, pieces=(), kind=jnp.bfloat16):
    entries = jax.random.normal(stream_key, dims, jnp.float32) * spread
    if len(pieces) > 0:
        entries = block_scale(stream_key, dims, pieces, -0.22, 0.18) * entries
    return jnp.clip(entries, min=-bound, max=bound).astype(kind)


def setup_inputs(seed: int = 0, part: int = 0) -> dict:
    keys = jax.random.split(jax.random.key(seed), 7)
    part_keys = jax.random.split(jax.random.fold_in(keys[6], part), 7)
    return {
        "image": normal_values(part_keys[0], (H, W, C), 1.0, 6.0, ((0, 8), (1, 2))),
        "tissue": place_ends((jax.random.randint(part_keys[1], (H // MB, W // MB), 0, 5) < 3).astype(jnp.int32), jax.random.fold_in(part_keys[1], 1), 0, 1),
        "first_kernel": normal_values(keys[2], (3, 3, C, C), (9 * C) ** -0.5, 0.1875),
        "first_bias": normal_values(keys[3], (C,), 0.5, 3.0, (), jnp.float32),
        "second_kernel": normal_values(keys[4], (3, 3, C, C), (9 * C) ** -0.5, 0.1875),
        "second_bias": normal_values(keys[5], (C,), 0.5, 3.0, (), jnp.float32),
    }


def conv_valid(padded, kernel, bias):
    rows = padded.shape[0] - 2
    cols = padded.shape[1] - 2
    chans = padded.shape[2]
    wide = jnp.concatenate([padded[:, 0:cols], padded[:, 1:cols + 1], padded[:, 2:cols + 2]], axis=-1)
    total = jnp.zeros((rows * cols, kernel.shape[3]), jnp.float32)
    for offset in range(3):
        block = wide[offset:offset + rows].reshape(rows * cols, 3 * chans)
        total = total + jnp.dot(block, kernel[offset].reshape(3 * chans, kernel.shape[3]), preferred_element_type=jnp.float32)
    return total.reshape(rows, cols, kernel.shape[3]) + bias


def reference(image, tissue, first_kernel, first_bias, second_kernel, second_bias):
    pixel_mask = jnp.repeat(jnp.repeat(tissue, MB, axis=0), MB, axis=1).astype(jnp.float32)[:, :, None]
    padded = jnp.pad(image, ((1, 1), (1, 1), (0, 0)))
    hidden = (jnp.maximum(conv_valid(padded, first_kernel, first_bias), 0.0) * pixel_mask).astype(jnp.bfloat16)
    padded = jnp.pad(hidden, ((1, 1), (1, 1), (0, 0)))
    return (jnp.maximum(conv_valid(padded, second_kernel, second_bias), 0.0) * pixel_mask).astype(jnp.bfloat16)
```

```python
import functools

import jax
import jax.numpy as jnp
from jax import lax
from jax.experimental import pallas as pl
from jax.experimental.pallas import tpu as pltpu
from jax.sharding import PartitionSpec as P

MB = 32
EDGE = 8
AROUND = [(dr, dc) for dr in (-1, 0, 1) for dc in (-1, 0, 1) if (dr, dc) != (0, 0)]


def largest_divisor(count, most):
    return max(d for d in range(1, most + 1) if count % d == 0)


def kernel(
    grid,
    img,
    tis,
    k1,
    b1,
    k2,
    b2,
    out,
    x,
    h,
    o,
    w1,
    w2,
    tiles,
    mask,
    load_sem,
    w_sem,
    out_sem,
    send_sem,
    recv_sem,
):
    n_rows, n_cols = grid
    rows, cols, chans = img.shape
    t_rows, t_cols = tis.shape[0], tis.shape[1]
    span = cols + 2 * EDGE
    r, c = lax.axis_index("rows"), lax.axis_index("cols")

    def has(dr, dc):
        ok = jnp.bool_(True)
        if dr:
            ok = ok & (r + dr >= 0) & (r + dr < n_rows)
        if dc:
            ok = ok & (c + dc >= 0) & (c + dc < n_cols)
        return ok

    def whom(dr, dc):
        where = {}
        if dr:
            where["rows"] = r + dr
        if dc:
            where["cols"] = c + dc
        return where

    to_rows = {-1: (0, 2), 0: (2, rows), 1: (rows + 2, 2)}
    to_cols = {-1: (cols + EDGE, EDGE), 0: (0, cols), 1: (cols, EDGE)}
    from_rows = {-1: (rows - 2, 2), 0: (0, rows), 1: (0, 2)}
    from_cols = {-1: (cols - EDGE, EDGE), 0: (0, cols), 1: (0, EDGE)}

    def place(dr, dc):
        return x.at[pl.ds(*to_rows[dr]), pl.ds(*to_cols[dc]), :]

    def copies(n, dr, dc):
        pixels = pltpu.make_async_remote_copy(
            src_ref=img.at[pl.ds(*from_rows[dr]), pl.ds(*from_cols[dc]), :],
            dst_ref=place(dr, dc),
            send_sem=send_sem.at[2 * n],
            recv_sem=recv_sem.at[2 * n],
            device_id=whom(-dr, -dc),
            device_id_type=pl.DeviceIdType.MESH,
        )
        tissue = pltpu.make_async_remote_copy(
            src_ref=tis,
            dst_ref=tiles.at[n],
            send_sem=send_sem.at[2 * n + 1],
            recv_sem=recv_sem.at[2 * n + 1],
            device_id=whom(-dr, -dc),
            device_id_type=pl.DeviceIdType.MESH,
        )
        return pixels, tissue

    barrier = pltpu.get_barrier_semaphore()
    for dr, dc in AROUND:

        @pl.when(has(dr, dc))
        def _():
            pl.semaphore_signal(
                barrier,
                inc=1,
                device_id=whom(dr, dc),
                device_id_type=pl.DeviceIdType.MESH,
            )

    load = pltpu.make_async_copy(img, place(0, 0), load_sem)
    load.start()
    weights = []
    for n, (k, w) in enumerate(((k1, w1), (k2, w2))):
        for half in (0, 1):
            weights.append(
                pltpu.make_async_copy(
                    k,
                    w.at[pl.ds(half, 3), :, :, pl.ds(half * chans, chans)],
                    w_sem.at[2 * n + half],
                )
            )
            weights[-1].start()
    for n, (dr, dc) in enumerate(AROUND):

        @pl.when(jnp.logical_not(has(dr, dc)))
        def _():
            at = (pl.ds(*to_rows[dr]), pl.ds(*to_cols[dc]))
            x[at] = jnp.zeros((to_rows[dr][1], to_cols[dc][1], chans), x.dtype)
            tiles[n] = jnp.zeros(tiles.shape[1:], tiles.dtype)

    present = [jnp.where(has(dr, dc), 1, 0) for dr, dc in AROUND]
    pl.semaphore_wait(barrier, sum(present))

    order = sorted(enumerate(AROUND), key=lambda p: (p[1][0] != 0, p[1][1] != 0))
    for n, (dr, dc) in order:

        @pl.when(has(-dr, -dc))
        def _():
            for copy in copies(n, dr, dc):
                copy.start()

    for w in (w1, w2):
        for s in range(3):
            w[3, s, :, :chans] = jnp.zeros((chans, chans), w.dtype)
            w[0, s, :, chans:] = jnp.zeros((chans, chans), w.dtype)

    def receive(which):
        for n, (dr, dc) in enumerate(AROUND):
            if (dr != 0) == which:

                @pl.when(has(dr, dc))
                def _():
                    for copy in copies(n, dr, dc):
                        copy.wait_recv()

    def put_mask(at, middle, right, left):
        for b in range(t_cols):
            mask[at, b * MB : (b + 1) * MB, :] = jnp.broadcast_to(
                middle[b : b + 1], (MB, chans)
            )
        mask[at, cols : cols + EDGE, :] = jnp.broadcast_to(right[0:1], (EDGE, chans))
        mask[at, cols + EDGE :, :] = jnp.broadcast_to(
            left[t_cols - 1 : t_cols], (EDGE, chans)
        )

    index = {d: n for n, d in enumerate(AROUND)}

    def conv(src, first, group, w, bias, emit):
        lhs = jnp.concatenate(
            [
                jnp.concatenate([src[first + 2 * g + k] for k in range(4)], axis=1)
                for g in range(group)
            ],
            axis=0,
        )
        parts = []
        for s in range(3):
            weight = w[:, s].reshape(4 * chans, 2 * chans)
            parts.append(jnp.dot(lhs, weight, preferred_element_type=jnp.float32))
        b = bias[...]
        for g in range(group):
            y = [p[g * span : (g + 1) * span] for p in parts]
            total = y[1] + pltpu.roll(y[0], 1, 0) + pltpu.roll(y[2], span - 1, 0)
            for half in (0, 1):
                value = total[:, half * chans : (half + 1) * chans] + b
                emit(first + 2 * g + half, jnp.maximum(value, 0.0))

    def hide(row, value):
        h[row] = (value * mask[(row + MB - 1) // MB]).astype(h.dtype)

    def show(row, value):
        o[row] = (value[:cols] * mask[row // MB + 1, :cols]).astype(o.dtype)

    receive(False)
    for t in range(t_rows):
        put_mask(1 + t, tis[t], tiles[index[0, 1], t], tiles[index[0, -1], t])
    load.wait()
    for copy in weights:
        copy.wait()

    inner1 = rows // 2 - 1
    g1 = largest_divisor(inner1, 3)

    def first_body(i, _):
        conv(x, 2 + 2 * g1 * i, g1, w1, b1, hide)
        return 0

    lax.fori_loop(0, inner1 // g1, first_body, 0)

    inner2 = rows // 2 - 2
    g2 = largest_divisor(inner2, 3)
    turns = inner2 // g2

    def put(i, start, length):
        at = pl.ds(start, length)
        return pltpu.make_async_copy(o.at[at], out.at[at], out_sem.at[i])

    def second_body(i, _):
        start = 2 + 2 * g2 * i
        conv(h, start, g2, w2, b2, show)
        put(i, start, 2 * g2).start()
        return 0

    lax.fori_loop(0, turns, second_body, 0)

    receive(True)
    for dr, at, t in ((-1, 0, t_rows - 1), (1, t_rows + 1, 0)):
        put_mask(
            at,
            tiles[index[dr, 0], t],
            tiles[index[dr, 1], t],
            tiles[index[dr, -1], t],
        )
    for row in (0, rows):
        conv(x, row, 1, w1, b1, hide)
    for n, row in enumerate((0, rows - 2)):
        conv(h, row, 1, w2, b2, show)
        put(turns + n, row, 2).start()

    for i in range(turns):
        put(i, 2 + 2 * g2 * i, 2 * g2).wait()
    for n, row in enumerate((0, rows - 2)):
        put(turns + n, row, 2).wait()
    for n, (dr, dc) in enumerate(AROUND):

        @pl.when(has(-dr, -dc))
        def _():
            for copy in copies(n, dr, dc):
                copy.wait_send()


def shards(image, tissue, first_kernel, first_bias, second_kernel, second_bias):
    rows, cols, chans = image.shape
    t_rows, t_cols = tissue.shape
    grid = (lax.axis_size("rows"), lax.axis_size("cols"))
    tis = jnp.broadcast_to(
        tissue.astype(jnp.float32)[:, :, None], (t_rows, t_cols, chans)
    )
    span = cols + 2 * EDGE
    vmem = pl.BlockSpec(memory_space=pltpu.VMEM)
    anywhere = pl.BlockSpec(memory_space=pl.ANY)
    return pl.pallas_call(
        functools.partial(kernel, grid),
        out_shape=jax.ShapeDtypeStruct((rows, cols, chans), jnp.bfloat16),
        in_specs=[anywhere, vmem, anywhere, vmem, anywhere, vmem],
        out_specs=anywhere,
        scratch_shapes=[
            pltpu.VMEM((rows + 4, span, chans), jnp.bfloat16),
            pltpu.VMEM((rows + 2, span, chans), jnp.bfloat16),
            pltpu.VMEM((rows, cols, chans), jnp.bfloat16),
            pltpu.VMEM((4, 3, chans, 2 * chans), jnp.bfloat16),
            pltpu.VMEM((4, 3, chans, 2 * chans), jnp.bfloat16),
            pltpu.VMEM((len(AROUND), t_rows, t_cols, chans), jnp.float32),
            pltpu.VMEM((t_rows + 2, span, chans), jnp.float32),
            pltpu.SemaphoreType.DMA,
            pltpu.SemaphoreType.DMA((4,)),
            pltpu.SemaphoreType.DMA((rows // 2,)),
            pltpu.SemaphoreType.DMA((2 * len(AROUND),)),
            pltpu.SemaphoreType.DMA((2 * len(AROUND),)),
        ],
        compiler_params=pltpu.CompilerParams(collective_id=0, has_side_effects=True),
    )(
        image,
        tis,
        first_kernel,
        first_bias.reshape(1, -1),
        second_kernel,
        second_bias.reshape(1, -1),
    )


def solution(mesh):
    in_specs = (
        P(("slides", "rows"), "cols", None),
        P(("slides", "rows"), "cols"),
        P(),
        P(),
        P(),
        P(),
    )
    out_specs = P(("slides", "rows"), "cols", None)
    return jax.shard_map(shards, mesh=mesh, in_specs=in_specs, out_specs=out_specs, check_vma=False)
```

```python
import functools

import jax
import jax.numpy as jnp
from jax import lax
from jax.experimental import pallas as pl
from jax.experimental.pallas import tpu as pltpu
from jax.sharding import PartitionSpec as P

MB = 32
VMEM_INNER = 32 * 2**20
VMEM_OUTER = 16 * 2**20
EDGE = 8
AROUND = [(dr, dc) for dr in (-1, 0, 1) for dc in (-1, 0, 1) if (dr, dc) != (0, 0)]


def largest_divisor(count, most):
    return max(d for d in range(1, most + 1) if count % d == 0)


def conv(src, firsts, w, bias, emit):
    span, chans = src.shape[1:]
    lhs = jnp.concatenate(
        [jnp.concatenate([src[f + k] for k in range(4)], axis=1) for f in firsts],
        axis=0,
    )
    parts = []
    for s in range(3):
        weight = w[:, s].reshape(4 * chans, 2 * chans)
        parts.append(jnp.dot(lhs, weight, preferred_element_type=jnp.float32))
    b = bias[...]
    for g, first in enumerate(firsts):
        y = [p[g * span : (g + 1) * span] for p in parts]
        total = y[1] + pltpu.roll(y[0], 1, 0) + pltpu.roll(y[2], span - 1, 0)
        for half in (0, 1):
            value = total[:, half * chans : (half + 1) * chans] + b
            emit(first + half, jnp.maximum(value, 0.0))


def inner_kernel(
    grid,
    img,
    tis_in,
    k1,
    b1_in,
    k2,
    b2_in,
    h,
    o,
    w2,
    mask,
    b2,
    x,
    w1,
    b1,
    tis,
    tiles,
    load_sem,
    w_sem,
    small_sem,
    send_sem,
    recv_sem,
):
    n_rows, n_cols = grid
    rows, cols, chans = img.shape
    t_rows, t_cols = tis.shape
    r, c = lax.axis_index("rows"), lax.axis_index("cols")

    def has(dr, dc):
        ok = jnp.bool_(True)
        if dr:
            ok = ok & (r + dr >= 0) & (r + dr < n_rows)
        if dc:
            ok = ok & (c + dc >= 0) & (c + dc < n_cols)
        return ok

    def whom(dr, dc):
        where = {}
        if dr:
            where["rows"] = r + dr
        if dc:
            where["cols"] = c + dc
        return where

    to_rows = {-1: (0, 2), 0: (2, rows), 1: (rows + 2, 2)}
    to_cols = {-1: (cols + EDGE, EDGE), 0: (0, cols), 1: (cols, EDGE)}
    from_rows = {-1: (rows, 2), 0: (2, rows), 1: (2, 2)}
    from_cols = {-1: (cols - EDGE, EDGE), 0: (0, cols), 1: (0, EDGE)}

    def pixels(n, dr, dc):
        return pltpu.make_async_remote_copy(
            src_ref=x.at[pl.ds(*from_rows[dr]), pl.ds(*from_cols[dc]), :],
            dst_ref=x.at[pl.ds(*to_rows[dr]), pl.ds(*to_cols[dc]), :],
            send_sem=send_sem.at[2 * n],
            recv_sem=recv_sem.at[2 * n],
            device_id=whom(-dr, -dc),
            device_id_type=pl.DeviceIdType.MESH,
        )

    def tissue(n, dr, dc):
        return pltpu.make_async_remote_copy(
            src_ref=tis,
            dst_ref=tiles.at[n],
            send_sem=send_sem.at[2 * n + 1],
            recv_sem=recv_sem.at[2 * n + 1],
            device_id=whom(-dr, -dc),
            device_id_type=pl.DeviceIdType.MESH,
        )

    barrier = pltpu.get_barrier_semaphore()
    for dr, dc in AROUND:

        @pl.when(has(dr, dc))
        def _():
            pl.semaphore_signal(
                barrier,
                inc=1,
                device_id=whom(dr, dc),
                device_id_type=pl.DeviceIdType.MESH,
            )

    loads = []
    for n, (start, length) in enumerate(((0, 2), (rows - 2, 2), (2, rows - 4))):
        loads.append(
            pltpu.make_async_copy(
                img.at[pl.ds(start, length)],
                x.at[pl.ds(2 + start, length), pl.ds(0, cols), :],
                load_sem.at[n],
            )
        )
        loads[-1].start()
    smalls = []
    for n, (src, dst) in enumerate(((tis_in, tis), (b1_in, b1), (b2_in, b2))):
        smalls.append(pltpu.make_async_copy(src, dst, small_sem.at[n]))
        smalls[-1].start()
    weights = []
    for n, (k, w) in enumerate(((k1, w1), (k2, w2))):
        for half in (0, 1):
            weights.append(
                pltpu.make_async_copy(
                    k,
                    w.at[pl.ds(half, 3), :, :, pl.ds(half * chans, chans)],
                    w_sem.at[2 * n + half],
                )
            )
            weights[-1].start()
    for n, (dr, dc) in enumerate(AROUND):

        @pl.when(jnp.logical_not(has(dr, dc)))
        def _():
            at = (pl.ds(*to_rows[dr]), pl.ds(*to_cols[dc]))
            x[at] = jnp.zeros((to_rows[dr][1], to_cols[dc][1], chans), x.dtype)
            tiles[n] = jnp.zeros(tiles.shape[1:], tiles.dtype)

    for copy in loads[:2]:
        copy.wait()
    smalls[0].wait()
    present = [jnp.where(has(dr, dc), 1, 0) for dr, dc in AROUND]
    pl.semaphore_wait(barrier, sum(present))

    def send(which, make):
        for n, (dr, dc) in enumerate(AROUND):
            if (dr != 0) == which:

                @pl.when(has(-dr, -dc))
                def _():
                    make(n, dr, dc).start()

    send(True, pixels)
    send(False, tissue)
    loads[2].wait()
    send(False, pixels)
    send(True, tissue)

    for w in (w1, w2):
        for s in range(3):
            w[3, s, :, :chans] = jnp.zeros((chans, chans), w.dtype)
            w[0, s, :, chans:] = jnp.zeros((chans, chans), w.dtype)

    def receive(which):
        for n, (dr, dc) in enumerate(AROUND):
            if (dr != 0) == which:

                @pl.when(has(dr, dc))
                def _():
                    tissue(n, dr, dc).wait_recv()
                    pixels(n, dr, dc).wait_recv()

    def put_mask(at, middle, right, left):
        def wide(values, b, length):
            value = values[:, b : b + 1].astype(jnp.float32)
            return jnp.broadcast_to(value, (length, chans))

        for b in range(t_cols):
            mask[at, b * MB : (b + 1) * MB, :] = wide(middle, b, MB)
        mask[at, cols : cols + EDGE, :] = wide(right, 0, EDGE)
        mask[at, cols + EDGE :, :] = wide(left, t_cols - 1, EDGE)

    index = {d: n for n, d in enumerate(AROUND)}

    def hide(row, value):
        h[row] = (value * mask[(row + MB - 1) // MB]).astype(h.dtype)

    def show(row, value):
        o[row] = (value[:cols] * mask[row // MB + 1, :cols]).astype(o.dtype)

    for copy in smalls[1:]:
        copy.wait()
    for copy in weights:
        copy.wait()
    receive(False)
    for t in range(t_rows):
        at = pl.ds(t, 1)
        put_mask(1 + t, tis[at], tiles[index[0, 1], at], tiles[index[0, -1], at])

    inner1 = rows // 2 - 1
    g1 = largest_divisor(inner1, 3)

    def first_body(i, _):
        conv(x, [2 + 2 * (g1 * i + g) for g in range(g1)], w1, b1, hide)
        return 0

    lax.fori_loop(0, inner1 // g1, first_body, 0)

    inner2 = rows // 2 - 2
    g2 = largest_divisor(inner2, 3)

    def second_body(i, _):
        conv(h, [2 + 2 * (g2 * i + g) for g in range(g2)], w2, b2, show)
        return 0

    lax.fori_loop(0, inner2 // g2, second_body, 0)

    receive(True)
    for dr, at, t in ((-1, 0, t_rows - 1), (1, t_rows + 1, 0)):
        put_mask(at, *[tiles[index[dr, dc], pl.ds(t, 1)] for dc in (0, 1, -1)])
    conv(x, [0, rows], w1, b1, hide)
    for n, (dr, dc) in enumerate(AROUND):

        @pl.when(has(-dr, -dc))
        def _():
            pixels(n, dr, dc).wait_send()
            tissue(n, dr, dc).wait_send()


def outer_kernel(h, o, w2, mask, b2, out, e, sem):
    rows, cols, _ = o.shape
    pieces = largest_divisor(rows - 4, 4)
    length = (rows - 4) // pieces
    copies = []
    for n in range(pieces):
        at = pl.ds(2 + n * length, length)
        copies.append(pltpu.make_async_copy(o.at[at], out.at[at], sem.at[n]))
        copies[-1].start()

    def show(row, value):
        at = row if row < 2 else row - rows + 4
        e[at] = (value[:cols] * mask[row // MB + 1, :cols]).astype(e.dtype)

    conv(h, [0, rows - 2], w2, b2, show)
    for n, row in enumerate((0, rows - 2)):
        copies.append(
            pltpu.make_async_copy(
                e.at[pl.ds(2 * n, 2)], out.at[pl.ds(row, 2)], sem.at[pieces + n]
            )
        )
        copies[-1].start()
    for copy in copies:
        copy.wait()


def shards(image, tissue, first_kernel, first_bias, second_kernel, second_bias):
    rows, cols, chans = image.shape
    t_rows, t_cols = tissue.shape
    grid = (lax.axis_size("rows"), lax.axis_size("cols"))
    span = cols + 2 * EDGE
    vmem = pl.BlockSpec(memory_space=pltpu.VMEM)
    anywhere = pl.BlockSpec(memory_space=pltpu.HBM)
    held = pl.pallas_call(
        functools.partial(inner_kernel, grid),
        out_shape=[
            pltpu.VMEM((rows + 2, span, chans), jnp.bfloat16),
            pltpu.VMEM((rows, cols, chans), jnp.bfloat16),
            pltpu.VMEM((4, 3, chans, 2 * chans), jnp.bfloat16),
            pltpu.VMEM((t_rows + 2, span, chans), jnp.float32),
            pltpu.VMEM((1, chans), jnp.float32),
        ],
        in_specs=[anywhere] * 6,
        out_specs=[vmem] * 5,
        scratch_shapes=[
            pltpu.VMEM((rows + 4, span, chans), jnp.bfloat16),
            pltpu.VMEM((4, 3, chans, 2 * chans), jnp.bfloat16),
            pltpu.VMEM((1, chans), jnp.float32),
            pltpu.VMEM((t_rows, t_cols), jnp.int32),
            pltpu.VMEM((len(AROUND), t_rows, t_cols), jnp.int32),
            pltpu.SemaphoreType.DMA((3,)),
            pltpu.SemaphoreType.DMA((4,)),
            pltpu.SemaphoreType.DMA((3,)),
            pltpu.SemaphoreType.DMA((2 * len(AROUND),)),
            pltpu.SemaphoreType.DMA((2 * len(AROUND),)),
        ],
        compiler_params=pltpu.CompilerParams(
            collective_id=0, has_side_effects=True, vmem_limit_bytes=VMEM_INNER
        ),
    )(
        *[
            pltpu.with_memory_space_constraint(value, pltpu.HBM)
            for value in (
                image,
                tissue,
                first_kernel,
                first_bias.reshape(1, -1),
                second_kernel,
                second_bias.reshape(1, -1),
            )
        ]
    )
    return pl.pallas_call(
        outer_kernel,
        out_shape=jax.ShapeDtypeStruct((rows, cols, chans), jnp.bfloat16),
        in_specs=[vmem] * 5,
        out_specs=anywhere,
        scratch_shapes=[
            pltpu.VMEM((4, cols, chans), jnp.bfloat16),
            pltpu.SemaphoreType.DMA((8,)),
        ],
        compiler_params=pltpu.CompilerParams(vmem_limit_bytes=VMEM_OUTER),
    )(*held)


def solution(mesh):
    in_specs = (
        P(("slides", "rows"), "cols", None),
        P(("slides", "rows"), "cols"),
        P(),
        P(),
        P(),
        P(),
    )
    out_specs = P(("slides", "rows"), "cols", None)
    return jax.shard_map(shards, mesh=mesh, in_specs=in_specs, out_specs=out_specs, check_vma=False)
```

```python
import functools

import jax
import jax.numpy as jnp
from jax import lax
from jax.experimental import pallas as pl
from jax.experimental.pallas import tpu as pltpu
from jax.sharding import PartitionSpec as P

MB = 32
VMEM_INNER = 32 * 2**20
VMEM_OUTER = 16 * 2**20
EDGE = 8
AROUND = [(dr, dc) for dr in (-1, 0, 1) for dc in (-1, 0, 1) if (dr, dc) != (0, 0)]


def largest_divisor(count, most):
    return max(d for d in range(1, most + 1) if count % d == 0)


def conv(src, firsts, w, bias, emit, pieces=None):
    pieces = pieces or ((0, src.shape[1]),)
    span, chans = sum(length for _, length in pieces), src.shape[2]
    lhs = jnp.concatenate(
        [
            jnp.concatenate(
                [src[f + k, start : start + length] for k in range(4)], axis=1
            )
            for f in firsts
            for start, length in pieces
        ],
        axis=0,
    )
    parts = []
    for s in range(3):
        weight = w[:, s].reshape(4 * chans, 2 * chans)
        parts.append(jnp.dot(lhs, weight, preferred_element_type=jnp.float32))
    b = bias[...]
    for g, first in enumerate(firsts):
        y = [p[g * span : (g + 1) * span] for p in parts]
        total = y[1] + pltpu.roll(y[0], 1, 0) + pltpu.roll(y[2], span - 1, 0)
        for half in (0, 1):
            value = total[:, half * chans : (half + 1) * chans] + b
            emit(first + half, jnp.maximum(value, 0.0))


def inner_kernel(
    grid,
    img,
    tis_in,
    k1,
    b1_in,
    k2,
    b2_in,
    h,
    o,
    w2,
    mask,
    b2,
    x,
    w1,
    b1,
    tis,
    tiles,
    load_sem,
    w_sem,
    small_sem,
    send_sem,
    recv_sem,
):
    n_rows, n_cols = grid
    rows, cols, chans = img.shape
    t_rows, t_cols = tis.shape
    r, c = lax.axis_index("rows"), lax.axis_index("cols")

    def has(dr, dc):
        ok = jnp.bool_(True)
        if dr:
            ok = ok & (r + dr >= 0) & (r + dr < n_rows)
        if dc:
            ok = ok & (c + dc >= 0) & (c + dc < n_cols)
        return ok

    def whom(dr, dc):
        where = {}
        if dr:
            where["rows"] = r + dr
        if dc:
            where["cols"] = c + dc
        return where

    to_rows = {-1: (0, 2), 0: (2, rows), 1: (rows + 2, 2)}
    to_cols = {-1: (cols + EDGE, EDGE), 0: (0, cols), 1: (cols, EDGE)}
    from_rows = {-1: (rows, 2), 0: (2, rows), 1: (2, 2)}
    from_cols = {-1: (cols - EDGE, EDGE), 0: (0, cols), 1: (0, EDGE)}

    def pixels(n, dr, dc):
        return pltpu.make_async_remote_copy(
            src_ref=x.at[pl.ds(*from_rows[dr]), pl.ds(*from_cols[dc]), :],
            dst_ref=x.at[pl.ds(*to_rows[dr]), pl.ds(*to_cols[dc]), :],
            send_sem=send_sem.at[2 * n],
            recv_sem=recv_sem.at[2 * n],
            device_id=whom(-dr, -dc),
            device_id_type=pl.DeviceIdType.MESH,
        )

    def tissue(n, dr, dc):
        return pltpu.make_async_remote_copy(
            src_ref=tis,
            dst_ref=tiles.at[n],
            send_sem=send_sem.at[2 * n + 1],
            recv_sem=recv_sem.at[2 * n + 1],
            device_id=whom(-dr, -dc),
            device_id_type=pl.DeviceIdType.MESH,
        )

    barrier = pltpu.get_barrier_semaphore()
    for dr, dc in AROUND:

        @pl.when(has(dr, dc))
        def _():
            pl.semaphore_signal(
                barrier,
                inc=1,
                device_id=whom(dr, dc),
                device_id_type=pl.DeviceIdType.MESH,
            )

    loads = []
    for n, (start, length) in enumerate(((0, 2), (rows - 2, 2), (2, rows - 4))):
        loads.append(
            pltpu.make_async_copy(
                img.at[pl.ds(start, length)],
                x.at[pl.ds(2 + start, length), pl.ds(0, cols), :],
                load_sem.at[n],
            )
        )
        loads[-1].start()
    smalls = []
    for n, (src, dst) in enumerate(((tis_in, tis), (b1_in, b1), (b2_in, b2))):
        smalls.append(pltpu.make_async_copy(src, dst, small_sem.at[n]))
        smalls[-1].start()
    weights = []
    for n, (k, w) in enumerate(((k1, w1), (k2, w2))):
        for half in (0, 1):
            weights.append(
                pltpu.make_async_copy(
                    k,
                    w.at[pl.ds(half, 3), :, :, pl.ds(half * chans, chans)],
                    w_sem.at[2 * n + half],
                )
            )
            weights[-1].start()
    for n, (dr, dc) in enumerate(AROUND):

        @pl.when(jnp.logical_not(has(dr, dc)))
        def _():
            at = (pl.ds(*to_rows[dr]), pl.ds(*to_cols[dc]))
            x[at] = jnp.zeros((to_rows[dr][1], to_cols[dc][1], chans), x.dtype)
            tiles[n] = jnp.zeros(tiles.shape[1:], tiles.dtype)

    for w in (w1, w2):
        for s in range(3):
            w[3, s, :, :chans] = jnp.zeros((chans, chans), w.dtype)
            w[0, s, :, chans:] = jnp.zeros((chans, chans), w.dtype)

    for copy in loads[:2]:
        copy.wait()
    smalls[0].wait()
    present = [jnp.where(has(dr, dc), 1, 0) for dr, dc in AROUND]
    pl.semaphore_wait(barrier, sum(present))

    def send(which, make):
        for n, (dr, dc) in enumerate(AROUND):
            if (dr != 0) == which:

                @pl.when(has(-dr, -dc))
                def _():
                    make(n, dr, dc).start()

    send(True, pixels)
    send(False, tissue)
    loads[2].wait()
    send(False, pixels)
    send(True, tissue)

    def receive(which):
        for n, (dr, dc) in enumerate(AROUND):
            if (dr != 0) == which:

                @pl.when(has(dr, dc))
                def _():
                    tissue(n, dr, dc).wait_recv()
                    pixels(n, dr, dc).wait_recv()

    def wide(values, b, length):
        value = values[:, b : b + 1].astype(jnp.float32)
        return jnp.broadcast_to(value, (length, chans))

    def put_middle(at, middle):
        for b in range(t_cols):
            mask[at, b * MB : (b + 1) * MB, :] = wide(middle, b, MB)

    def put_sides(at, right, left):
        mask[at, cols : cols + EDGE, :] = wide(right, 0, EDGE)
        mask[at, cols + EDGE :, :] = wide(left, t_cols - 1, EDGE)

    index = {d: n for n, d in enumerate(AROUND)}

    def hide(row, value):
        h[row] = (value * mask[(row + MB - 1) // MB]).astype(h.dtype)

    def hide_middle(row, value):
        value = value * mask[(row + MB - 1) // MB, :cols]
        h[row, :cols] = value.astype(h.dtype)

    tile = 2 * EDGE
    strip = ((cols - tile, tile), (cols, tile), (0, tile))
    early = lax.broadcasted_iota(jnp.int32, (tile, chans), 0) < EDGE

    def hide_strip(row, value):
        for n, (start, length) in enumerate(strip):
            at = pl.ds(start, length)
            new = value[n * tile : (n + 1) * tile] * mask[(row + MB - 1) // MB, at]
            if n != 1:
                old = h[row, at].astype(jnp.float32)
                new = jnp.where(early, *((old, new) if n == 0 else (new, old)))
            h[row, at] = new.astype(h.dtype)

    def show(row, value):
        o[row] = (value[:cols] * mask[row // MB + 1, :cols]).astype(o.dtype)

    for copy in smalls[1:]:
        copy.wait()
    for copy in weights:
        copy.wait()
    for t in range(t_rows):
        put_middle(1 + t, tis[pl.ds(t, 1)])

    inner1 = rows // 2 - 1
    g1 = largest_divisor(inner1, 5)

    def first_body(i, _):
        firsts = [2 + 2 * (g1 * i + g) for g in range(g1)]
        conv(x, firsts, w1, b1, hide_middle, ((0, cols),))
        return 0

    lax.fori_loop(0, inner1 // g1, first_body, 0)

    receive(False)
    for t in range(t_rows):
        at = pl.ds(t, 1)
        put_sides(1 + t, tiles[index[0, 1], at], tiles[index[0, -1], at])
    g3 = largest_divisor(inner1, 15)

    def strip_body(i, _):
        firsts = [2 + 2 * (g3 * i + g) for g in range(g3)]
        conv(x, firsts, w1, b1, hide_strip, strip)
        return 0

    lax.fori_loop(0, inner1 // g3, strip_body, 0)

    inner2 = rows // 2 - 2
    g2 = largest_divisor(inner2, 7)

    def second_body(i, _):
        conv(h, [2 + 2 * (g2 * i + g) for g in range(g2)], w2, b2, show)
        return 0

    lax.fori_loop(0, inner2 // g2, second_body, 0)

    receive(True)
    for dr, at, t in ((-1, 0, t_rows - 1), (1, t_rows + 1, 0)):
        put_middle(at, tiles[index[dr, 0], pl.ds(t, 1)])
        put_sides(at, *[tiles[index[dr, dc], pl.ds(t, 1)] for dc in (1, -1)])
    conv(x, [0, rows], w1, b1, hide)
    for n, (dr, dc) in enumerate(AROUND):

        @pl.when(has(-dr, -dc))
        def _():
            pixels(n, dr, dc).wait_send()
            tissue(n, dr, dc).wait_send()


def outer_kernel(h, o, w2, mask, b2, out, e, sem):
    rows, cols, _ = o.shape
    pieces = largest_divisor(rows - 4, 4)
    length = (rows - 4) // pieces
    copies = []
    for n in range(pieces):
        at = pl.ds(2 + n * length, length)
        copies.append(pltpu.make_async_copy(o.at[at], out.at[at], sem.at[n]))
        copies[-1].start()

    def show(row, value):
        at = row if row < 2 else row - rows + 4
        e[at] = (value[:cols] * mask[row // MB + 1, :cols]).astype(e.dtype)

    conv(h, [0, rows - 2], w2, b2, show)
    for n, row in enumerate((0, rows - 2)):
        copies.append(
            pltpu.make_async_copy(
                e.at[pl.ds(2 * n, 2)], out.at[pl.ds(row, 2)], sem.at[pieces + n]
            )
        )
        copies[-1].start()
    for copy in copies:
        copy.wait()


def shards(image, tissue, first_kernel, first_bias, second_kernel, second_bias):
    rows, cols, chans = image.shape
    t_rows, t_cols = tissue.shape
    grid = (lax.axis_size("rows"), lax.axis_size("cols"))
    span = cols + 2 * EDGE
    vmem = pl.BlockSpec(memory_space=pltpu.VMEM)
    anywhere = pl.BlockSpec(memory_space=pltpu.HBM)
    held = pl.pallas_call(
        functools.partial(inner_kernel, grid),
        out_shape=[
            pltpu.VMEM((rows + 2, span, chans), jnp.bfloat16),
            pltpu.VMEM((rows, cols, chans), jnp.bfloat16),
            pltpu.VMEM((4, 3, chans, 2 * chans), jnp.bfloat16),
            pltpu.VMEM((t_rows + 2, span, chans), jnp.float32),
            pltpu.VMEM((1, chans), jnp.float32),
        ],
        in_specs=[anywhere] * 6,
        out_specs=[vmem] * 5,
        scratch_shapes=[
            pltpu.VMEM((rows + 4, span, chans), jnp.bfloat16),
            pltpu.VMEM((4, 3, chans, 2 * chans), jnp.bfloat16),
            pltpu.VMEM((1, chans), jnp.float32),
            pltpu.VMEM((t_rows, t_cols), jnp.int32),
            pltpu.VMEM((len(AROUND), t_rows, t_cols), jnp.int32),
            pltpu.SemaphoreType.DMA((3,)),
            pltpu.SemaphoreType.DMA((4,)),
            pltpu.SemaphoreType.DMA((3,)),
            pltpu.SemaphoreType.DMA((2 * len(AROUND),)),
            pltpu.SemaphoreType.DMA((2 * len(AROUND),)),
        ],
        compiler_params=pltpu.CompilerParams(
            collective_id=0, has_side_effects=True, vmem_limit_bytes=VMEM_INNER
        ),
    )(
        *[
            pltpu.with_memory_space_constraint(value, pltpu.HBM)
            for value in (
                image,
                tissue,
                first_kernel,
                first_bias.reshape(1, -1),
                second_kernel,
                second_bias.reshape(1, -1),
            )
        ]
    )
    return pl.pallas_call(
        outer_kernel,
        out_shape=jax.ShapeDtypeStruct((rows, cols, chans), jnp.bfloat16),
        in_specs=[vmem] * 5,
        out_specs=anywhere,
        scratch_shapes=[
            pltpu.VMEM((4, cols, chans), jnp.bfloat16),
            pltpu.SemaphoreType.DMA((8,)),
        ],
        compiler_params=pltpu.CompilerParams(vmem_limit_bytes=VMEM_OUTER),
    )(*held)


def solution(mesh):
    in_specs = (
        P(("slides", "rows"), "cols", None),
        P(("slides", "rows"), "cols"),
        P(),
        P(),
        P(),
        P(),
    )
    out_specs = P(("slides", "rows"), "cols", None)
    return jax.shard_map(shards, mesh=mesh, in_specs=in_specs, out_specs=out_specs, check_vma=False)
```
